512 devices in a mesh: dev: 512 (over z, y, x, core).
Axes of the slice: x: 4, y: 8, z: 8, core: 2. Of those that a mesh axis runs over, the one named last changes fastest.
Arguments:
- image_feats: bfloat16 [6144, 1152], P('dev'), may hold values from -0.1875 to 0.1875
- text_feats: bfloat16 [6144, 1152], P('dev'), may hold values from -0.1875 to 0.1875
- image_head: bfloat16 [1152, 640], replicated, may hold values from -0.1875 to 0.1875
- text_head: bfloat16 [1152, 640], replicated, may hold values from -0.1875 to 0.1875
- log_scale: float32 [], replicated, may hold values from 1.6 to 2.3
- logit_bias: float32 [], replicated, may hold values from -8 to -4
- image_group: int32 [6144], P('dev'), may hold values from 0 to 3071
- text_group: int32 [6144], P('dev'), may hold values from 0 to 3071
Outputs:
- loss: float32 [], replicated
- grad_images: bfloat16 [6144, 1152], P('dev')
- grad_texts: bfloat16 [6144, 1152], P('dev')
- grad_scale: float32 [], replicated
- grad_bias: float32 [], replicated
The draws below stay inside these ranges and needn't reach their ends.
All inputs are finite; a program needn't handle non-finite values.
Results may differ from the reference program's by a relative error of at most 0.0063.
Values may be sent and summed in bfloat16 or wider, within the bound.
A program may use at most 128 MiB of HBM per device.

```python
import jax
import jax.numpy as jnp
from jax import lax

D = 1152
E = 640
PAIRS = 6144


def touch_ends(entries, own_key, low, largest):
    longest = entries.shape.index(max(entries.shape))
    spots = []
    for shift in (0, 1):
        where = [jax.random.randint(jax.random.fold_in(own_key, axis), (), 0, length) for axis, length in enumerate(entries.shape)]
        where[longest] = (where[longest] + shift) % entries.shape[longest]
        spots.append(tuple(where))
    return entries.at[spots[0]].set(low).at[spots[1]].set(largest)


def levels(own_key, extent, shards, low, largest):
    loudness, own = 1.0, jax.random.fold_in(own_key, 6)
    for dim, blocks in shards:
        steps = jnp.exp(jax.random.uniform(jax.random.fold_in(own, dim), (blocks,), jnp.float32, low / len(shards), largest / len(shards)))
        loudness = loudness * jnp.repeat(steps, extent[dim] // blocks).reshape([-1 if axis == dim else 1 for axis in range(len(extent))])
    return loudness


def gaussian(own_key, extent, deviation, reach, shards=(), dtype=jnp.bfloat16):
    gain = levels(own_key, extent, shards, -0.22, 0.18) if shards else 1.0
    array = jax.random.normal(own_key, extent, jnp.float32) * deviation * gain
    return jnp.minimum(jnp.maximum(array, -reach), reach).astype(dtype)


def setup_inputs(seed: int = 0) -> dict:
    streams_of = jax.random.split(jax.random.key(seed), 9)
    image_feats = gaussian(streams_of[0], (PAIRS, D), 0.03, 0.1875, ((0, 512),))
    text_feats = gaussian(streams_of[1], (PAIRS, D), 0.03, 0.1875, ((0, 512),))
    image_head = gaussian(streams_of[2], (D, E), D ** -0.5, 0.1875)
    text_head = gaussian(streams_of[3], (D, E), D ** -0.5, 0.1875)
    log_scale = jnp.clip(jax.random.uniform(streams_of[4], (), jnp.float32, 1.6, 2.3), 1.6, 2.3)
    logit_bias = jnp.clip(jax.random.uniform(streams_of[5], (), jnp.float32, -8.0, -4.0), -8.0, -4.0)
    image_group = touch_ends(jax.random.randint(streams_of[6], (PAIRS,), 0, PAIRS // 2), jax.random.fold_in(streams_of[6], 1), 0, (PAIRS // 2) - 1).astype(jnp.int32)
    text_group = touch_ends(jax.random.randint(streams_of[7], (PAIRS,), 0, PAIRS // 2), jax.random.fold_in(streams_of[7], 1), 0, (PAIRS // 2) - 1).astype(jnp.int32)
    return {"image_feats": image_feats, "text_feats": text_feats, "image_head": image_head, "text_head": text_head, "log_scale": log_scale, "logit_bias": logit_bias, "image_group": image_group, "text_group": text_group}


epsilon = 1e-06

def normalize(projected):
    length = jnp.sqrt(lax.optimization_barrier(jnp.sum(projected * projected, axis=1, keepdims=True)) + epsilon)
    return (projected / length, length)

def backward_rows(grad_unit, unit_vec, length, weights):
    inner = lax.optimization_barrier(jnp.sum(unit_vec * grad_unit, axis=1, keepdims=True))
    grad_proj = ((grad_unit - unit_vec * inner) / length).astype(jnp.bfloat16)
    return jnp.dot(grad_proj, weights.T, preferred_element_type=jnp.float32).astype(jnp.bfloat16)

def reference(image_feats, text_feats, image_head, text_head, log_scale, logit_bias, image_group, text_group):
    img_unit, img_length = normalize(jnp.dot(image_feats, image_head, preferred_element_type=jnp.float32))
    txt_unit, txt_length = normalize(jnp.dot(text_feats, text_head, preferred_element_type=jnp.float32))
    img_emb = img_unit.astype(jnp.bfloat16)
    txt_emb = txt_unit.astype(jnp.bfloat16)
    logit_scale = jnp.exp(log_scale)
    cosine = jnp.dot(img_emb, txt_emb.T, preferred_element_type=jnp.float32)
    label_sign = jnp.where(image_group[:, None] == text_group[None, :], 1.0, -1.0).astype(jnp.float32)
    margin = label_sign * (logit_scale * cosine + logit_bias)
    total = jnp.sum(jax.nn.softplus(-margin))
    slopes = -label_sign * jax.nn.sigmoid(-margin)
    slope_low = slopes.astype(jnp.bfloat16)
    grad_img_unit = logit_scale * jnp.dot(slope_low, txt_emb, preferred_element_type=jnp.float32)
    grad_txt_unit = logit_scale * jnp.dot(slope_low.T, img_emb, preferred_element_type=jnp.float32)
    pairs = image_feats.shape[0]
    loss = total / pairs
    grad_scale = logit_scale * jnp.sum(slopes * cosine) / pairs
    grad_bias = jnp.sum(slopes) / pairs
    grad_images = backward_rows(grad_img_unit, img_unit, img_length, image_head)
    grad_texts = backward_rows(grad_txt_unit, txt_unit, txt_length, text_head)
    return (loss, grad_images, grad_texts, grad_scale, grad_bias)
```

```python
import functools

import jax
import jax.numpy as jnp
from jax import lax
from jax.experimental import pallas as pl
from jax.experimental.pallas import tpu as pltpu
from jax.sharding import Mesh
from jax.sharding import PartitionSpec as P

DEV = ("dev_0", "dev_1", "dev_2", "dev_3")
RING = 8
ROWS = 12
PAD = 16
D = 1152
E = 640
W = E + 128
PAIRS = 6144
NEAR = (4, 3, 5, 2, 6, 1, 7)

EPS = 1e-6
F32 = jnp.float32
BF16 = jnp.bfloat16


def nt(a, b):
    return lax.dot_general(a, b, (((1,), (1,)), ((), ())), preferred_element_type=F32)


def nn(a, b):
    return lax.dot_general(a, b, (((1,), (0,)), ((), ())), preferred_element_type=F32)


def tn(a, b):
    return lax.dot_general(a, b, (((0,), (0,)), ((), ())), preferred_element_type=F32)


def id_features(ids, image_side):
    shape = (PAD, 128)
    row = lax.broadcasted_iota(jnp.int32, shape, 0)
    lane = lax.broadcasted_iota(jnp.int32, shape, 1)
    value = jnp.zeros(shape, jnp.int32)
    for r in range(ROWS):
        value = jnp.where(row == r, ids[r], value)
    high, low = value >> 6, value & 63
    square = high * high + low * low
    upper = jnp.where(row < ROWS, square >> 6, -192)
    lower = square & 63
    one, many = jnp.ones(shape, jnp.int32), jnp.full(shape, 64, jnp.int32)
    if image_side:
        parts = (high, low, upper, lower, many, one)
    else:
        parts = (-2 * high, -2 * low, many, one, upper, lower)
    out = jnp.zeros(shape, jnp.int32)
    for k, part in enumerate(parts):
        out = jnp.where(lane == k, part, out)
    return out.astype(F32).astype(BF16)


def project(feats, head):
    proj = nn(feats[...], head[...])
    length = jnp.sqrt(jnp.sum(proj * proj, axis=1, keepdims=True) + EPS)
    return proj / length, length


def kernel(
    ifeat, tfeat, ihead_hbm, thead_hbm, log_scale, logit_bias, igroup, tgroup,
    loss_o, gimg_o, gtxt_o, gscale_o, gbias_o,
    ihead, thead, iemb, temb, iown, town, cos_s, dist_s, slope_s, acc_i, acc_t,
    part_i, part_t, core_rx, mid_i, mid_t, x_rx_i, x_rx_t, ring_i, ring_t,
    sums_v, sum_z, sum_y, sum_c,
    head_sem, s_g1i, r_g1i, s_g1t, r_g1t, s_x, r_x, s_core, r_core,
    s_r1i, r_r1i, s_r1t, r_r1t, s_sz, r_sz, s_sy, r_sy, s_sc, r_sc,
):
    z, y, x, c = (lax.axis_index(a) for a in DEV)
    odd = lax.rem(x, 2)
    x_hi = lax.rem(x + 3 + 2 * odd, 4)
    x_lo = x + 1 - 2 * odd
    other = 1 - c

    head_copies = [
        pltpu.make_async_copy(ihead_hbm, ihead, head_sem.at[0]),
        pltpu.make_async_copy(thead_hbm, thead, head_sem.at[1]),
    ]
    for copy in head_copies:
        copy.start()

    rz = [lax.rem(z + k, RING) for k in NEAR]
    ry = [lax.rem(y + k, RING) for k in NEAR]
    cluster = [(lax.rem(x + dx, 4), lax.rem(c + dc, 2)) for dx in range(4) for dc in range(2) if (dx, dc) != (0, 0)]

    barrier = pltpu.get_barrier_semaphore()
    for t in rz:
        pl.semaphore_signal(barrier, inc=1, device_id={"dev_0": t})
    for t in ry:
        pl.semaphore_signal(barrier, inc=1, device_id={"dev_1": t})
    for tx, tc in cluster:
        pl.semaphore_signal(barrier, inc=1, device_id={"dev_2": tx, "dev_3": tc})

    def send(src, dst, ssem, rsem, device):
        copy = pltpu.make_async_remote_copy(src, dst, ssem, rsem, device_id=device)
        copy.start()
        return copy

    sent = []

    iown[...] = jnp.zeros_like(iown)
    town[...] = jnp.zeros_like(town)
    iown[:, E:] = id_features(igroup, True)
    town[:, E:] = id_features(tgroup, False)
    head_copies[0].wait()
    img_unit, img_len = project(ifeat, ihead)
    iown[0:ROWS, 0:E] = img_unit.astype(BF16)
    iemb[0, z] = iown[...]
    pl.semaphore_wait(barrier, 21)
    for k, t in enumerate(rz):
        sent.append(send(iown, iemb.at[0, z], s_g1i.at[k], r_g1i.at[z], {"dev_0": t}))
    head_copies[1].wait()
    txt_unit, txt_len = project(tfeat, thead)
    town[0:ROWS, 0:E] = txt_unit.astype(BF16)
    temb[0, 0, y] = town[...]
    for k, t in enumerate(ry):
        sent.append(send(town, temb.at[0, 0, y], s_g1t.at[k], r_g1t.at[y], {"dev_1": t}))

    def arrived(dst, rsem):
        pltpu.make_async_copy(dst, dst, rsem).wait()

    for t in rz[::-1]:
        arrived(iemb.at[0, t], r_g1i.at[t])
    sent.append(send(iemb.at[0], iemb.at[1], s_x.at[0], r_x.at[0], {"dev_2": x_hi}))
    for t in ry[::-1]:
        arrived(temb.at[0, 0, t], r_g1t.at[t])
    sent.append(send(temb.at[0, 0], temb.at[0, 1], s_x.at[1], r_x.at[1], {"dev_2": x_lo}))
    sent.append(send(temb.at[0, 0], temb.at[1, 0], s_core.at[0], r_core.at[0], {"dev_3": other}))
    arrived(temb.at[0, 1], r_x.at[1])
    sent.append(send(temb.at[0, 1], temb.at[1, 1], s_core.at[1], r_core.at[1], {"dev_3": other}))
    arrived(iemb.at[1], r_x.at[0])

    scale_row = jnp.exp(jnp.full((1, 256), log_scale[0], F32))
    bias = logit_bias[0]
    n_img = 2 * RING * PAD
    images = iemb.at[...]

    def pair_block(h, totals):
        ie = iemb[...].reshape(n_img, W)
        te = temb[h].reshape(n_img, W)
        cos_s[...] = nt(ie[:, :E], te[:, :E])
        dist_s[...] = nt(ie[:, E:], te[:, E:])
        step = 32

        def rows(i, totals):
            at = pl.ds(pl.multiple_of(i * step, step), step)
            cosine = cos_s[at, :]
            dist = dist_s[at, :]
            match = dist < 0.5
            valid = dist > -0.5
            logit = scale_row * cosine + bias
            minus = jnp.where(match, -logit, logit)
            small = jnp.exp(-jnp.abs(minus))
            ratio = 1.0 / (1.0 + small)
            sig = jnp.where(minus >= 0, ratio, small * ratio)
            slope = jnp.where(valid, jnp.where(match, -sig, sig), 0.0)
            soft = jnp.where(valid, jnp.maximum(minus, 0.0) + jnp.log1p(small), 0.0)
            slope_s[at, :] = slope.astype(BF16)
            fold = lambda a: a[0:8] + a[8:16] + a[16:24] + a[24:32]
            return (
                totals[0] + fold(soft),
                totals[1] + fold(slope * cosine),
                totals[2] + fold(slope),
            )

        totals = lax.fori_loop(0, n_img // step, rows, totals)
        slope = slope_s[...]
        grad_i = nn(slope, te[:, :E])
        grad_t = tn(slope, ie[:, :E])
        return grad_i, grad_t, totals

    zero = jnp.zeros((8, 256), F32)
    totals = (zero, zero, zero)
    grad_i, grad_t, totals = pair_block(0, totals)
    acc_i[...] = grad_i
    acc_t[...] = grad_t
    arrived(temb.at[1, 0], r_core.at[0])
    arrived(temb.at[1, 1], r_core.at[1])
    grad_i, grad_t, totals = pair_block(1, totals)
    part_t[...] = grad_t.astype(BF16).reshape(2, RING, PAD, E)
    sent.append(send(part_t, core_rx, s_core.at[2], r_core.at[2], {"dev_3": other}))
    grad_i = (grad_i + acc_i[...]).reshape(2, RING, PAD, E)
    part_i[...] = grad_i[1].astype(BF16)
    acc_i[...] = grad_i.reshape(n_img, E)
    sent.append(send(part_i, x_rx_i, s_x.at[2], r_x.at[2], {"dev_2": x_hi}))

    lanes = [t[:, 0:128] + t[:, 128:256] for t in totals]
    mine = jnp.concatenate([jnp.sum(t, axis=0, keepdims=True) for t in lanes] + [jnp.zeros((5, 128), F32)], axis=0)
    sums_v[0] = mine
    sum_z[z] = mine
    for k, t in enumerate(rz):
        sent.append(send(sums_v.at[0], sum_z.at[z], s_sz.at[k], r_sz.at[z], {"dev_0": t}))

    arrived(core_rx, r_core.at[2])
    grad_t = acc_t[...].reshape(2, RING, PAD, E) + core_rx[...].astype(F32)
    mid_t[...] = grad_t[1].astype(BF16)
    acc_t[0 : RING * PAD] = grad_t[0].reshape(RING * PAD, E)
    sent.append(send(mid_t, x_rx_t, s_x.at[3], r_x.at[3], {"dev_2": x_lo}))

    arrived(x_rx_i, r_x.at[2])
    mid_i[...] = (acc_i[0 : RING * PAD].reshape(RING, PAD, E) + x_rx_i[...].astype(F32)).astype(BF16)
    ring_i[z] = mid_i[z]
    for k, t in enumerate(rz):
        sent.append(send(mid_i.at[t], ring_i.at[z], s_r1i.at[k], r_r1i.at[z], {"dev_0": t}))

    for t in rz:
        arrived(sum_z.at[t], r_sz.at[t])
    mine = functools.reduce(lambda a, b: a + b, [sum_z[k] for k in range(RING)])
    sums_v[1] = mine
    sum_y[y] = mine
    for k, t in enumerate(ry):
        sent.append(send(sums_v.at[1], sum_y.at[y], s_sy.at[k], r_sy.at[y], {"dev_1": t}))

    arrived(x_rx_t, r_x.at[3])
    part_b = acc_t[0 : RING * PAD].reshape(RING, PAD, E) + x_rx_t[...].astype(F32)
    part_t2 = part_b.astype(BF16)
    core_rx[0] = part_t2
    ring_t[y] = core_rx[0, y]
    for k, t in enumerate(ry):
        sent.append(send(core_rx.at[0, t], ring_t.at[y], s_r1t.at[k], r_r1t.at[y], {"dev_1": t}))

    for t in ry:
        arrived(sum_y.at[t], r_sy.at[t])
    mine = functools.reduce(lambda a, b: a + b, [sum_y[k] for k in range(RING)])
    sums_v[2] = mine
    sum_c[2 * x + c] = mine
    for k, (tx, tc) in enumerate(cluster):
        sent.append(send(sums_v.at[2], sum_c.at[2 * x + c], s_sc.at[k], r_sc.at[2 * x + c], {"dev_2": tx, "dev_3": tc}))

    scale_e = jnp.exp(jnp.full((1, E), log_scale[0], F32))

    def backward(ring, unit, length, head, out):
        grad = functools.reduce(lambda a, b: a + b, [ring[k].astype(F32) for k in range(RING)])
        grad = scale_e * grad[0:ROWS]
        inner = jnp.sum(unit * grad, axis=1, keepdims=True)
        low = ((grad - unit * inner) / length).astype(BF16)
        out[...] = nt(low, head[...]).astype(BF16)

    for t in rz[::-1]:
        arrived(ring_i.at[t], r_r1i.at[t])
    backward(ring_i, img_unit, img_len, ihead, gimg_o)
    for t in ry[::-1]:
        arrived(ring_t.at[t], r_r1t.at[t])
    backward(ring_t, txt_unit, txt_len, thead, gtxt_o)

    for tx, tc in cluster:
        arrived(sum_c.at[2 * tx + tc], r_sc.at[2 * tx + tc])
    mine = functools.reduce(lambda a, b: a + b, [sum_c[k] for k in range(8)])
    whole = jnp.sum(mine, axis=1, keepdims=True) / PAIRS
    scale_1 = jnp.exp(jnp.full((1, 1), log_scale[0], F32))
    loss_o[...] = whole[0:1]
    gscale_o[...] = scale_1 * whole[1:2]
    gbias_o[...] = whole[2:3]

    for copy in sent:
        copy.wait_send()


def on_device(ifeat, tfeat, ihead, thead, log_scale, logit_bias, igroup, tgroup):
    vmem = pl.BlockSpec(memory_space=pltpu.VMEM)
    smem = pl.BlockSpec(memory_space=pltpu.SMEM)
    hbm = pl.BlockSpec(memory_space=pl.ANY)
    dma = pltpu.SemaphoreType.DMA
    blocks = RING * PAD
    one = jax.ShapeDtypeStruct((1, 1), F32)
    grad = jax.ShapeDtypeStruct((ROWS, D), BF16)
    loss, gimg, gtxt, gscale, gbias = pl.pallas_call(
        kernel,
        out_shape=(one, grad, grad, one, one),
        in_specs=[vmem, vmem, hbm, hbm, smem, smem, smem, smem],
        out_specs=[vmem] * 5,
        scratch_shapes=[
            pltpu.VMEM((D, E), BF16),
            pltpu.VMEM((D, E), BF16),
            pltpu.VMEM((2, RING, PAD, W), BF16),
            pltpu.VMEM((2, 2, RING, PAD, W), BF16),
            pltpu.VMEM((PAD, W), BF16),
            pltpu.VMEM((PAD, W), BF16),
            pltpu.VMEM((2 * blocks, 2 * blocks), F32),
            pltpu.VMEM((2 * blocks, 2 * blocks), F32),
            pltpu.VMEM((2 * blocks, 2 * blocks), BF16),
            pltpu.VMEM((2 * blocks, E), F32),
            pltpu.VMEM((2 * blocks, E), F32),
            pltpu.VMEM((RING, PAD, E), BF16),
            pltpu.VMEM((2, RING, PAD, E), BF16),
            pltpu.VMEM((2, RING, PAD, E), BF16),
            pltpu.VMEM((RING, PAD, E), BF16),
            pltpu.VMEM((RING, PAD, E), BF16),
            pltpu.VMEM((RING, PAD, E), BF16),
            pltpu.VMEM((RING, PAD, E), BF16),
            pltpu.VMEM((RING, PAD, E), BF16),
            pltpu.VMEM((RING, PAD, E), BF16),
            pltpu.VMEM((3, 8, 128), F32),
            pltpu.VMEM((RING, 8, 128), F32),
            pltpu.VMEM((RING, 8, 128), F32),
            pltpu.VMEM((RING, 8, 128), F32),
            dma((2,)),
            dma((7,)), dma((8,)), dma((7,)), dma((8,)),
            dma((4,)), dma((4,)), dma((3,)), dma((3,)),
            dma((7,)), dma((8,)), dma((7,)), dma((8,)),
            dma((7,)), dma((8,)), dma((7,)), dma((8,)), dma((7,)), dma((8,)),
        ],
        compiler_params=pltpu.CompilerParams(collective_id=0, has_side_effects=True),
    )(ifeat, tfeat, ihead, thead, log_scale.reshape(1), logit_bias.reshape(1), igroup, tgroup)
    return loss[0, 0], gimg, gtxt, gscale[0, 0], gbias[0, 0]


def solution(mesh):
    torus = Mesh(mesh.devices.reshape(8, 8, 4, 2), DEV)
    return jax.shard_map(
        on_device,
        mesh=torus,
        in_specs=(P(DEV, None), P(DEV, None), P(), P(), P(), P(), P(DEV), P(DEV)),
        out_specs=(P(), P(DEV, None), P(DEV, None), P(), P()),
        check_vma=False,
    )
```

```python
import functools

import jax
import jax.numpy as jnp
from jax import lax
from jax.experimental import pallas as pl
from jax.experimental.pallas import tpu as pltpu
from jax.sharding import Mesh
from jax.sharding import PartitionSpec as P

DEV = ("dev_0", "dev_1", "dev_2", "dev_3")
RING = 8
ROWS = 12
PAD = 16
D = 1152
E = 640
PAIRS = 6144
NEAR = (4, 3, 5, 2, 6, 1, 7)

EPS = 1e-6
F32 = jnp.float32
BF16 = jnp.bfloat16


def nt(a, b):
    return lax.dot_general(a, b, (((1,), (1,)), ((), ())), preferred_element_type=F32)


def nn(a, b):
    return lax.dot_general(a, b, (((1,), (0,)), ((), ())), preferred_element_type=F32)


def tn(a, b):
    return lax.dot_general(a, b, (((0,), (0,)), ((), ())), preferred_element_type=F32)


def id_features(ids, image_side):
    shape = (PAD, 128)
    row = lax.broadcasted_iota(jnp.int32, shape, 0)
    lane = lax.broadcasted_iota(jnp.int32, shape, 1)
    value = jnp.zeros(shape, jnp.int32)
    for r in range(ROWS):
        value = jnp.where(row == r, ids[r], value)
    high, low = value >> 6, value & 63
    square = high * high + low * low
    upper = jnp.where(row < ROWS, square >> 6, -192)
    lower = square & 63
    one, many = jnp.ones(shape, jnp.int32), jnp.full(shape, 64, jnp.int32)
    if image_side:
        parts = (high, low, upper, lower, many, one)
    else:
        parts = (-2 * high, -2 * low, many, one, upper, lower)
    out = jnp.zeros(shape, jnp.int32)
    for k, part in enumerate(parts):
        out = jnp.where(lane == k, part, out)
    return out.astype(F32).astype(BF16)


def project(feats, head):
    proj = nn(feats[...], head[...])
    length = jnp.sqrt(jnp.sum(proj * proj, axis=1, keepdims=True) + EPS)
    return proj / length, length


def kernel(
    ifeat_hbm, tfeat_hbm, ihead_hbm, thead_hbm, log_scale, logit_bias, igroup_hbm, tgroup_hbm,
    gimg_o, gtxt_o, sums_o,
    igroup, tgroup,
    ifeat, tfeat, ihead, thead, iemb, temb, iid, tid, iown, town, iid_own, tid_own,
    cos_s, dist_s, slope_s, acc_i, acc_t,
    part_i, part_t, core_rx, mid_i, send_t, mid_t, x_rx_i, x_rx_t, ring_i, ring_t,
    sums_v, sum_z, sum_y, sum_c,
    load_sem, s_ring, r_g1i, r_g1t, s_small, r_id, s_x, r_x, s_core, r_core,
    r_r2i, r_r2t, r_r1, r_sum,
):
    z, y, x, c = (lax.axis_index(a) for a in DEV)
    odd = lax.rem(x, 2)
    x_hi = lax.rem(x + 3 + 2 * odd, 4)
    x_lo = x + 1 - 2 * odd
    other = 1 - c

    rz = [lax.rem(z + k, RING) for k in NEAR]
    ry = [lax.rem(y + k, RING) for k in NEAR]
    fz = [lax.rem(z + RING - k, RING) for k in NEAR]
    fy = [lax.rem(y + RING - k, RING) for k in NEAR]
    cluster = [(lax.rem(x + dx, 4), lax.rem(c + dc, 2)) for dx in range(4) for dc in range(2) if (dx, dc) != (0, 0)]

    barrier = pltpu.get_barrier_semaphore()
    for t in rz:
        pl.semaphore_signal(barrier, inc=1, device_id={"dev_0": t})
    for t in ry:
        pl.semaphore_signal(barrier, inc=1, device_id={"dev_1": t})
    for tx, tc in cluster:
        pl.semaphore_signal(barrier, inc=1, device_id={"dev_2": tx, "dev_3": tc})

    loads = [
        pltpu.make_async_copy(a, b, load_sem.at[k])
        for k, (a, b) in enumerate(((ifeat_hbm, ifeat), (ihead_hbm, ihead), (tfeat_hbm, tfeat), (thead_hbm, thead),
                                     (igroup_hbm, igroup), (tgroup_hbm, tgroup)))
    ]
    for copy in loads:
        copy.start()

    def send(src, dst, ssem, rsem, device):
        pltpu.make_async_remote_copy(src, dst, ssem, rsem, device_id=device).start()

    def arrived(dst, rsem):
        pltpu.make_async_copy(dst, dst, rsem).wait()

    for copy in loads[4:]:
        copy.wait()
    iown[...] = jnp.zeros_like(iown)
    town[...] = jnp.zeros_like(town)
    iid_own[...] = id_features(igroup, True)
    tid_own[...] = id_features(tgroup, False)
    iid[0, z] = iid_own[...]
    tid[0, 0, y] = tid_own[...]
    loads[0].wait()
    loads[1].wait()
    img_unit, img_len = project(ifeat, ihead)
    iown[0:ROWS, :] = img_unit.astype(BF16)
    iemb[0, z] = iown[...]
    pl.semaphore_wait(barrier, 21)
    for k, t in enumerate(rz):
        send(iown, iemb.at[0, z], s_ring.at[0], r_g1i.at[z], {"dev_0": t})
    send(iown, iemb.at[1, z], s_x.at[0], r_x.at[0], {"dev_2": x_hi})
    loads[2].wait()
    loads[3].wait()
    txt_unit, txt_len = project(tfeat, thead)
    town[0:ROWS, :] = txt_unit.astype(BF16)
    temb[0, 0, y] = town[...]
    for k, t in enumerate(ry):
        send(town, temb.at[0, 0, y], s_ring.at[1], r_g1t.at[y], {"dev_1": t})
    send(town, temb.at[0, 1, y], s_x.at[1], r_x.at[1], {"dev_2": x_lo})
    for k, t in enumerate(rz):
        send(iid_own, iid.at[0, z], s_small.at[0], r_id.at[0], {"dev_0": t})
    for k, t in enumerate(ry):
        send(tid_own, tid.at[0, 0, y], s_small.at[1], r_id.at[1], {"dev_1": t})

    for k in range(7):
        arrived(iemb.at[0, fz[k]], r_g1i.at[fz[k]])
        send(iemb.at[0, fz[k]], iemb.at[1, fz[k]], s_x.at[0], r_x.at[0], {"dev_2": x_hi})
        arrived(temb.at[0, 0, fy[k]], r_g1t.at[fy[k]])
        send(temb.at[0, 0, fy[k]], temb.at[0, 1, fy[k]], s_x.at[1], r_x.at[1], {"dev_2": x_lo})
    send(temb.at[0, 0], temb.at[1, 0], s_core.at[0], r_core.at[0], {"dev_3": other})
    arrived(iid.at[0, pl.ds(0, 7)], r_id.at[0])
    send(iid.at[0], iid.at[1], s_small.at[2], r_id.at[2], {"dev_2": x_hi})
    arrived(tid.at[0, 0, pl.ds(0, 7)], r_id.at[1])
    send(tid.at[0, 0], tid.at[0, 1], s_small.at[3], r_id.at[3], {"dev_2": x_lo})
    arrived(temb.at[0, 1], r_x.at[1])
    send(temb.at[0, 1], temb.at[1, 1], s_core.at[1], r_core.at[1], {"dev_3": other})
    arrived(tid.at[0, 1], r_id.at[3])
    send(tid.at[0], tid.at[1], s_core.at[3], r_core.at[3], {"dev_3": other})
    arrived(iemb.at[1], r_x.at[0])
    arrived(iid.at[1], r_id.at[2])

    scale_row = jnp.exp(jnp.full((1, 256), log_scale[0], F32))
    bias = logit_bias[0]
    n_img = 2 * RING * PAD

    def pair_block(h, totals):
        ie = iemb[...].reshape(n_img, E)
        te = temb[h].reshape(n_img, E)
        cos_s[...] = nt(ie, te)
        dist_s[...] = nt(iid[...].reshape(n_img, 128), tid[h].reshape(n_img, 128))
        step = 32

        def rows(i, totals):
            at = pl.ds(pl.multiple_of(i * step, step), step)
            cosine = cos_s[at, :]
            dist = dist_s[at, :]
            match = dist < 0.5
            valid = dist > -0.5
            logit = scale_row * cosine + bias
            minus = jnp.where(match, -logit, logit)
            small = jnp.exp(-jnp.abs(minus))
            ratio = 1.0 / (1.0 + small)
            sig = jnp.where(minus >= 0, ratio, small * ratio)
            slope = jnp.where(valid, jnp.where(match, -sig, sig), 0.0)
            soft = jnp.where(valid, jnp.maximum(minus, 0.0) + jnp.log1p(small), 0.0)
            slope_s[at, :] = slope.astype(BF16)
            fold = lambda a: a[0:8] + a[8:16] + a[16:24] + a[24:32]
            return (
                totals[0] + fold(soft),
                totals[1] + fold(slope * cosine),
                totals[2] + fold(slope),
            )

        totals = lax.fori_loop(0, n_img // step, rows, totals)
        slope = slope_s[...]
        return nn(slope, te), tn(slope, ie), totals

    zero = jnp.zeros((8, 256), F32)
    totals = (zero, zero, zero)
    grad_i, grad_t, totals = pair_block(0, totals)
    acc_i[...] = grad_i
    acc_t[...] = grad_t.reshape(2, RING, PAD, E)
    arrived(temb.at[1, 0], r_core.at[0])
    arrived(temb.at[1, 1], r_core.at[1])
    arrived(tid.at[1], r_core.at[3])
    grad_i, grad_t, totals = pair_block(1, totals)
    part_t[...] = grad_t.astype(BF16).reshape(2, RING, PAD, E)
    send(part_t, core_rx, s_core.at[2], r_core.at[2], {"dev_3": other})
    lanes = [t[:, 0:128] + t[:, 128:256] for t in totals]
    mine = jnp.concatenate([jnp.sum(t, axis=0, keepdims=True) for t in lanes] + [jnp.zeros((5, 128), F32)], axis=0)
    sums_v[0] = mine
    sum_c[2 * x + c] = mine
    for k, (tx, tc) in enumerate(cluster):
        send(sums_v.at[0], sum_c.at[2 * x + c], s_small.at[4], r_sum.at[0], {"dev_2": tx, "dev_3": tc})
    grad_i = (grad_i + acc_i[...]).reshape(2, RING, PAD, E)
    part_i[...] = grad_i[1].astype(BF16)
    acc_i[...] = grad_i.reshape(n_img, E)
    order_z = rz + [z]
    order_y = ry + [y]
    for k, t in enumerate(order_z):
        send(part_i.at[t], x_rx_i.at[t], s_x.at[2], r_r2i.at[t], {"dev_2": x_hi})

    arrived(core_rx, r_core.at[2])
    grad_t = acc_t[...] + core_rx[...].astype(F32)
    send_t[...] = grad_t[1].astype(BF16)
    acc_t[0] = grad_t[0]
    for k, t in enumerate(order_y):
        send(send_t.at[t], x_rx_t.at[t], s_x.at[3], r_r2t.at[t], {"dev_2": x_lo})

    arrived(sum_c.at[pl.ds(0, 7)], r_sum.at[0])
    mine = functools.reduce(lambda a, b: a + b, [sum_c[k] for k in range(8)])
    sums_v[1] = mine
    sum_z[z] = mine
    for k, t in enumerate(rz):
        send(sums_v.at[1], sum_z.at[z], s_small.at[5], r_sum.at[1], {"dev_0": t})

    for k, t in enumerate(order_z):
        arrived(x_rx_i.at[t], r_r2i.at[t])
        at = pl.ds(pl.multiple_of(t * PAD, PAD), PAD)
        block = (acc_i[at, :] + x_rx_i[t].astype(F32)).astype(BF16)
        if k < 7:
            mid_i[t] = block
            send(mid_i.at[t], ring_i.at[z], s_ring.at[2], r_r1.at[0], {"dev_0": t})
        else:
            ring_i[z] = block
    for k, t in enumerate(order_y):
        arrived(x_rx_t.at[t], r_r2t.at[t])
        block = (acc_t[0, t] + x_rx_t[t].astype(F32)).astype(BF16)
        if k < 7:
            mid_t[t] = block
            send(mid_t.at[t], ring_t.at[y], s_ring.at[3], r_r1.at[1], {"dev_1": t})
        else:
            ring_t[y] = block

    arrived(sum_z.at[pl.ds(0, 7)], r_sum.at[1])
    mine = functools.reduce(lambda a, b: a + b, [sum_z[k] for k in range(RING)])
    sums_v[2] = mine
    sum_y[y] = mine
    for k, t in enumerate(ry):
        send(sums_v.at[2], sum_y.at[y], s_small.at[6], r_sum.at[2], {"dev_1": t})

    scale_e = jnp.exp(jnp.full((1, E), log_scale[0], F32))

    def backward(ring, unit, length, head, out):
        grad = functools.reduce(lambda a, b: a + b, [ring[k].astype(F32) for k in range(RING)])
        grad = scale_e * grad[0:ROWS]
        inner = jnp.sum(unit * grad, axis=1, keepdims=True)
        low = ((grad - unit * inner) / length).astype(BF16)
        out[...] = nt(low, head[...]).astype(BF16)

    arrived(ring_i.at[pl.ds(0, 7)], r_r1.at[0])
    backward(ring_i, img_unit, img_len, ihead, gimg_o)
    arrived(ring_t.at[pl.ds(0, 7)], r_r1.at[1])
    backward(ring_t, txt_unit, txt_len, thead, gtxt_o)

    arrived(sum_y.at[pl.ds(0, 7)], r_sum.at[2])
    total = functools.reduce(lambda a, b: a + b, [sum_y[k] for k in range(RING)])
    row = lax.broadcasted_iota(jnp.int32, (8, 128), 0)
    sums_o[...] = total * jnp.where(row == 1, jnp.exp(jnp.full((8, 128), log_scale[0], F32)), 1.0)

    seven = pl.ds(0, 7)
    arrived(iemb.at[0, seven], s_ring.at[0])
    arrived(temb.at[0, 0, seven], s_ring.at[1])
    arrived(mid_i.at[seven], s_ring.at[2])
    arrived(mid_t.at[seven], s_ring.at[3])
    arrived(iid.at[0, seven], s_small.at[0])
    arrived(tid.at[0, 0, seven], s_small.at[1])
    arrived(iid.at[0], s_small.at[2])
    arrived(tid.at[0, 0], s_small.at[3])
    for k, part in enumerate((sum_c, sum_z, sum_y)):
        arrived(part.at[seven], s_small.at[4 + k])
    arrived(iemb.at[0], s_x.at[0])
    arrived(temb.at[0, 0], s_x.at[1])
    arrived(part_i, s_x.at[2])
    arrived(send_t, s_x.at[3])
    arrived(temb.at[0, 0], s_core.at[0])
    arrived(temb.at[0, 1], s_core.at[1])
    arrived(part_t, s_core.at[2])
    arrived(tid.at[0], s_core.at[3])


def finish(gimg, gtxt, sums, loss_o, gimg_o, gtxt_o, gscale_o, gbias_o):
    gimg_o[...] = gimg[...]
    gtxt_o[...] = gtxt[...]
    whole = jnp.sum(sums[...], axis=1, keepdims=True) / PAIRS
    loss_o[...] = whole[0:1]
    gscale_o[...] = whole[1:2]
    gbias_o[...] = whole[2:3]


def on_device(ifeat, tfeat, ihead, thead, log_scale, logit_bias, igroup, tgroup):
    vmem = pl.BlockSpec(memory_space=pltpu.VMEM)
    smem = pl.BlockSpec(memory_space=pltpu.SMEM)
    hbm = pl.BlockSpec(memory_space=pltpu.HBM)
    dma = pltpu.SemaphoreType.DMA
    blocks = RING * PAD
    one = jax.ShapeDtypeStruct((1, 1), F32)
    grad = jax.ShapeDtypeStruct((ROWS, D), BF16)
    ring = pltpu.VMEM((RING, PAD, E), BF16)
    two_rings = pltpu.VMEM((2, RING, PAD, E), BF16)
    small = pltpu.VMEM((RING, 8, 128), F32)
    arrays = (ifeat, tfeat, ihead, thead, igroup, tgroup)
    ifeat, tfeat, ihead, thead, igroup, tgroup = [pltpu.with_memory_space_constraint(a, pltpu.HBM) for a in arrays]
    gimg, gtxt, sums = pl.pallas_call(
        kernel,
        out_shape=(grad, grad, jax.ShapeDtypeStruct((8, 128), F32)),
        in_specs=[hbm, hbm, hbm, hbm, smem, smem, hbm, hbm],
        out_specs=[vmem] * 3,
        scratch_shapes=[
            pltpu.SMEM((ROWS,), jnp.int32),
            pltpu.SMEM((ROWS,), jnp.int32),
            pltpu.VMEM((ROWS, D), BF16),
            pltpu.VMEM((ROWS, D), BF16),
            pltpu.VMEM((D, E), BF16),
            pltpu.VMEM((D, E), BF16),
            two_rings,
            pltpu.VMEM((2, 2, RING, PAD, E), BF16),
            pltpu.VMEM((2, RING, PAD, 128), BF16),
            pltpu.VMEM((2, 2, RING, PAD, 128), BF16),
            pltpu.VMEM((PAD, E), BF16),
            pltpu.VMEM((PAD, E), BF16),
            pltpu.VMEM((PAD, 128), BF16),
            pltpu.VMEM((PAD, 128), BF16),
            pltpu.VMEM((2 * blocks, 2 * blocks), F32),
            pltpu.VMEM((2 * blocks, 2 * blocks), F32),
            pltpu.VMEM((2 * blocks, 2 * blocks), BF16),
            pltpu.VMEM((2 * blocks, E), F32),
            pltpu.VMEM((2, RING, PAD, E), F32),
            ring, two_rings, two_rings, ring, ring, ring, ring, ring, ring, ring,
            pltpu.VMEM((3, 8, 128), F32),
            small, small, small,
            dma((6,)), dma((4,)), dma((8,)), dma((8,)), dma((7,)), dma((4,)), dma((4,)), dma((2,)), dma((4,)), dma((4,)),
            dma((8,)), dma((8,)), dma((2,)), dma((3,)),
        ],
        compiler_params=pltpu.CompilerParams(
            collective_id=0, has_side_effects=True, vmem_limit_bytes=24 << 20
        ),
    )(ifeat, tfeat, ihead, thead, log_scale.reshape(1), logit_bias.reshape(1), igroup, tgroup)
    loss, gimg, gtxt, gscale, gbias = pl.pallas_call(
        finish,
        out_shape=(one, grad, grad, one, one),
        in_specs=[vmem] * 3,
        out_specs=[vmem] * 5,
        compiler_params=pltpu.CompilerParams(vmem_limit_bytes=4 << 20),
    )(gimg, gtxt, sums)
    return loss[0, 0], gimg, gtxt, gscale[0, 0], gbias[0, 0]


def solution(mesh):
    torus = Mesh(mesh.devices.reshape(8, 8, 4, 2), DEV)
    return jax.shard_map(
        on_device,
        mesh=torus,
        in_specs=(P(DEV, None), P(DEV, None), P(), P(), P(), P(), P(DEV), P(DEV)),
        out_specs=(P(), P(DEV, None), P(DEV, None), P(), P()),
        check_vma=False,
    )
```
